32 devices in a mesh: cls: 4 (over y, x), org: 8 (over z, core).
Axes of the slice: x: 2, y: 2, z: 4, core: 2. Of those that a mesh axis runs over, the one named last changes fastest.
Arguments:
- flows_start: float32 [8, 49152], P('cls', 'org'), may hold values from 150 to 300
- interaction: float32 [8, 8, 49152], P('cls', None, 'org'), may hold values from 0.2 to 2
- free_time: float32 [8, 49152], P('cls', 'org'), may hold values from 0.01 to 0.1
- capacity: float32 [49152], P('org'), may hold values from 300 to 900
- demand: int32 [8, 8, 60], P('cls', 'org'), may hold values from 0 to 15
- incidence: int32 [2, 8, 8, 2, 49152], P(None, 'cls', 'org'), may hold values from 0 to 1073741823, as said below
- step_size: float32 [2], replicated, may hold values from 0.3 to 0.6
Outputs:
- flows: float32 [8, 49152], P('cls', 'org')
- costs: float32 [8, 49152], P('cls', 'org')
- skims: float32 [2, 8, 8, 60], P(None, 'cls', 'org')
- gaps: float32 [2], replicated
The draws below stay inside these ranges and needn't reach their ends.
Inputs may be any that keep to these rules, and one draw needn't show every extreme that they name: Bit b of incidence[k, c, o, w, l] tells whether link l lies on class c's path from anchor o to destination w * 30 + b in iteration k; each path is the union of 4 runs of 64 consecutive links (counted cyclically over the links) at drawn starts, the first of which is shared by all 30 destinations of one word.
All inputs are finite; a program needn't handle non-finite values.
Results may differ from the reference program's by a relative error of at most 0.0013.
Values sent between devices are 32-bit elements; how exact they have to be, the bound alone decides.
A program may use at most 256 MiB of HBM per device.

```python
import math
import jax
import jax.numpy as jnp
from jax import lax

C = 8
BITS = 30
DWORDS = 2
LINK_DEV = 6144
ITERS = 2
RUNS = 4
SEG = 64
ANCHORS = 8
DEST = 60
LINKS = 49152
N_ORG = 8


def draw_incidence(key, part):
    own_starts = jax.random.randint(jax.random.fold_in(key, 11), (BITS, ITERS, C, ANCHORS, DWORDS, RUNS - 1), 0, LINKS).astype(jnp.int32)
    shared = jax.random.randint(jax.random.fold_in(key, 23), (1, ITERS, C, ANCHORS, DWORDS, 1), 0, LINKS).astype(jnp.int32)
    shared_all = jnp.broadcast_to(shared, (BITS, ITERS, C, ANCHORS, DWORDS, 1))
    starts = jnp.concatenate([shared_all, own_starts], axis=-1)
    link_ids = jnp.arange(LINKS, dtype=jnp.int32)

    def add_bit(bit_number, words):
        chosen = lax.dynamic_index_in_dim(starts, bit_number, 0, keepdims=False)
        inside = jnp.zeros(words.shape, jnp.bool_)
        for run_index in range(RUNS):
            offset = jnp.mod(link_ids - chosen[..., run_index, None], LINKS)
            inside = jnp.logical_or(inside, offset < SEG)
        return words + jnp.left_shift(inside.astype(jnp.int32), bit_number)
    empty = jnp.zeros((ITERS, C, ANCHORS, DWORDS, LINKS), jnp.int32)
    return lax.fori_loop(0, BITS, add_bit, empty)


def plant(result, rng, low, top_value):
    place = [jax.random.randint(jax.random.fold_in(rng, axis), (), 0, length) for axis, length in enumerate(result.shape)]
    widest = result.shape.index(max(result.shape))
    next_to = place[:widest] + [(place[widest] + 1) % result.shape[widest]] + place[widest + 1:]
    return result.at[tuple(place)].set(low).at[tuple(next_to)].set(top_value)


def shard_levels(own_key, dims, split, low, top_value):
    factor_of = 1.0
    for position, shards_of in split:
        draws = jax.random.uniform(jax.random.fold_in(jax.random.fold_in(own_key, 6), position), (shards_of,), jnp.float32, low / len(split), top_value / len(split))
        factor_of = factor_of * jnp.repeat(jnp.exp(draws), dims[position] // shards_of).reshape((-1,) + (1,) * (len(dims) - 1 - position))
    return factor_of


def setup_inputs(seed: int = 0) -> dict:
    seeds = jax.random.split(jax.random.key(seed), 8)
    return {
        "flows_start": jnp.clip(150.0 + 150.0 * jax.random.uniform(seeds[0], (C, LINKS), jnp.float32) ** shard_levels(seeds[0], (C, LINKS), ((0, 4), (1, 8)), -0.2, 0.2), 150.0, 300.0),
        "interaction": jnp.clip(jnp.exp(math.log(2.0) - 2.3025851 * jax.random.uniform(seeds[1], (C, C, LINKS), jnp.float32) ** shard_levels(seeds[1], (C, C, LINKS), ((0, 4), (2, 8)), -0.2, 0.2)), 0.2, 2.0),
        "free_time": jnp.clip(jnp.exp(math.log(0.1) - 2.3025851 * jax.random.uniform(seeds[2], (C, LINKS), jnp.float32) ** shard_levels(seeds[2], (C, LINKS), ((0, 4), (1, 8)), -0.2, 0.2)), 0.01, 0.1),
        "capacity": jnp.clip(300.0 + 600.0 * jax.random.uniform(seeds[3], (LINKS,), jnp.float32) ** shard_levels(seeds[3], (LINKS,), ((0, 8),), -0.2, 0.2), 300.0, 900.0),
        "demand": plant(jax.random.randint(seeds[4], (C, ANCHORS, DEST), 0, 16), jax.random.fold_in(seeds[4], 1), 0, 15).astype(jnp.int32),
        "incidence": draw_incidence(jax.random.fold_in(seeds[7], 71), 0),
        "step_size": jnp.clip(jax.random.uniform(seeds[6], (ITERS,), jnp.float32, 0.3, 0.6), 0.3, 0.6),
    }


HIGH = lax.Precision.HIGHEST


def unpack(packed):
    shifts = jnp.arange(BITS, dtype=jnp.int32)
    bit_table = jnp.bitwise_and(jnp.right_shift(packed[..., :, None, :], shifts[:, None]), 1)
    new_shape = packed.shape[:-2] + (packed.shape[-2] * BITS, packed.shape[-1])
    return bit_table.reshape(new_shape).astype(jnp.float32)


def link_cost(flows_all, inter, free, cap):
    load_sum = jnp.einsum("cel,el->cl", inter, flows_all, precision=HIGH)
    load_ratio = load_sum / cap
    square = load_ratio * load_ratio
    return free * (1.0 + 0.15 * square * square)


def reference(flows_start, interaction, free_time, capacity, demand, incidence, step_size):
    demand_real = demand.astype(jnp.float32)
    flow_now = flows_start
    skim_list = []
    gap_list = []
    for iteration in range(ITERS):
        cost_now = link_cost(flow_now, interaction, free_time, capacity)
        skim_rows = []
        load_rows = []
        for class_index in range(C):
            packed_all = incidence[iteration, class_index]
            times_row = cost_now[class_index]
            trips = demand_real[class_index]

            def advance(skim_sum, block_index):
                first = block_index * LINK_DEV
                word_block = lax.dynamic_slice_in_dim(packed_all, first, LINK_DEV, 2)
                bit_table = unpack(word_block)
                cost_block = lax.dynamic_slice_in_dim(times_row, first, LINK_DEV, 0)
                skim_sum = skim_sum + jnp.einsum("odl,l->od", bit_table, cost_block, precision=HIGH)
                load_block = jnp.einsum("od,odl->l", trips, bit_table, precision=HIGH)
                return skim_sum, load_block

            skim_sum, load_blocks = lax.scan(advance, jnp.zeros((ANCHORS, DEST), jnp.float32), jnp.arange(N_ORG, dtype=jnp.int32))
            skim_rows.append(skim_sum)
            load_rows.append(load_blocks.reshape(LINKS))
        skim_now = jnp.stack(skim_rows)
        aon = jnp.stack(load_rows)
        cost_total = jnp.sum(cost_now * flow_now)
        path_total = jnp.sum(demand_real * skim_now)
        gap_list.append((cost_total - path_total) / cost_total)
        skim_list.append(skim_now)
        flow_now = flow_now + step_size[iteration] * (aon - flow_now)
    cost_final = link_cost(flow_now, interaction, free_time, capacity)
    return flow_now, cost_final, jnp.stack(skim_list), jnp.stack(gap_list)
```

```python
import functools

import jax
import jax.numpy as jnp
from jax import lax
from jax.experimental import pallas as pl
from jax.experimental.pallas import tpu as pltpu
from jax.sharding import PartitionSpec as P

BITS = 30
TRIP_BITS = 4
LANES = 128
SUB = 8
MESH = pl.DeviceIdType.MESH


def kernel(
    n_cls, n_org, iters, class_local, words, link_rows,
    flow_ref, inter_ref, free_ref, cap_ref, demand_ref, inc_ref, step_ref,
    flow_out, cost_out, skim_out, gap_out,
    flows_all, aon_own, aon_pair, pair_buf, rs_buf, aon_total, times, acc, part_one, part_two,
    flow_send, flow_recv, pair_send, pair_recv, rs_send, rs_recv,
    time_send, time_recv, fwd_send, fwd_recv, one_send, one_recv, two_send, two_recv,
):
    half = n_org // 2
    my_cls = lax.axis_index("cls")
    my_org = lax.axis_index("org")
    my_z = my_org // 2
    core = my_org % 2
    other = 1 - core
    partner = my_z * 2 + other
    groups = link_rows // SUB
    class_count = n_cls * class_local

    barrier = pltpu.get_barrier_semaphore()
    for i in range(1, n_org):
        pl.semaphore_signal(barrier, inc=1, device_id={"org": (my_org + i) % n_org}, device_id_type=MESH)
    for i in range(1, n_cls):
        pl.semaphore_signal(barrier, inc=1, device_id={"cls": (my_cls + i) % n_cls}, device_id_type=MESH)

    demand = demand_ref[...]
    lane = lax.broadcasted_iota(jnp.int32, demand.shape, 1)
    spot = lane % BITS
    low_half = BITS // 2
    masks = {}
    for bit in range(TRIP_BITS):
        chosen = jnp.bitwise_and(jnp.right_shift(demand, bit), 1)
        for w in range(words):
            inside = lane // BITS == w
            low = jnp.where(inside & (spot < low_half), jnp.left_shift(chosen, spot % low_half), 0)
            high = jnp.where(inside & (spot >= low_half), jnp.left_shift(chosen, spot % low_half), 0)
            low_sum = jnp.sum(low.astype(jnp.float32), axis=1, keepdims=True).astype(jnp.int32)
            high_sum = jnp.sum(high.astype(jnp.float32), axis=1, keepdims=True).astype(jnp.int32)
            both = low_sum + jnp.left_shift(high_sum, low_half)
            for c in range(class_local):
                masks[bit, w, c] = jnp.broadcast_to(both[c:c + 1, :], (SUB, LANES))

    def aon_chunks(k, parity, dest):
        def one(j, carry):
            target = 2 * ((my_z + j) % half) + parity
            base = target * (link_rows * words)
            for c in range(class_local):
                for g in range(groups):
                    word = [
                        inc_ref[k, c, pl.ds(base + g * SUB * words + w, SUB, stride=words), :]
                        for w in range(words)
                    ]
                    total = None
                    for bit in range(TRIP_BITS):
                        count = None
                        for w in range(words):
                            ones = lax.population_count(jnp.bitwise_and(word[w], masks[bit, w, c]))
                            count = ones if count is None else count + ones
                        count = jnp.left_shift(count, bit)
                        total = count if total is None else total + count
                    dest[k, j, c, g * SUB:(g + 1) * SUB, :] = total.astype(jnp.float32)
            return carry

        lax.fori_loop(0, half, one, 0)

    def copy(src, dst, send, recv, device):
        made = pltpu.make_async_remote_copy(
            src_ref=src, dst_ref=dst, send_sem=send, recv_sem=recv, device_id=device, device_id_type=MESH
        )
        made.start()
        return made

    def pair_copy(k):
        return copy(aon_pair.at[k], pair_buf.at[k], pair_send.at[k], pair_recv.at[k], {"org": partner})

    def flow_copies(k, src):
        return [
            copy(src, flows_all.at[k, my_cls], flow_send.at[k, i], flow_recv.at[k, i], {"cls": (my_cls + i) % n_cls})
            for i in range(1, n_cls)
        ]

    def rs_copies(k):
        return [
            copy(aon_own.at[k, j], rs_buf.at[k, j], rs_send.at[k, j], rs_recv.at[k, j],
                 {"org": 2 * ((my_z + j) % half) + core})
            for j in range(1, half)
        ]

    def time_copies(k):
        made = [copy(times.at[k, 0, 0], times.at[k, 0, 1], time_send.at[k, 0], time_recv.at[k, 0], {"org": partner})]
        for j in range(1, half):
            made.append(
                copy(times.at[k, 0, 0], times.at[k, j, 0], time_send.at[k, j], time_recv.at[k, j],
                     {"org": 2 * ((my_z + j) % half) + core})
            )
        return made

    def forward(k, j):
        return copy(times.at[k, j, 0], times.at[k, j, 1], fwd_send.at[k, j], fwd_recv.at[k, j], {"org": partner})

    def flow_of(k, c):
        return flows_all[k, my_cls, pl.ds(c, link_rows, stride=class_local), :]

    def link_time(k, c):
        load = None
        for e in range(class_count):
            weight = inter_ref[c, pl.ds(e, link_rows, stride=class_count), :]
            flow = flows_all[k, e // class_local, pl.ds(e % class_local, link_rows, stride=class_local), :]
            term = weight * flow
            load = term if load is None else load + term
        ratio = load / cap_ref[...]
        square = ratio * ratio
        return free_ref[pl.ds(c, link_rows, stride=class_local), :] * (1.0 + 0.15 * square * square)

    def fold_rows(value):
        return jnp.sum(value.reshape(groups, SUB, LANES), axis=0)

    def skim_chunk(k, j, p, first):
        source = 2 * ((my_z + half - j) % half) + (core if p == 0 else other)
        base = source * (link_rows * words)
        for c in range(class_local):
            cost = [times[k, j, p, c, g * SUB:(g + 1) * SUB, :] for g in range(groups)]
            for w in range(words):
                word = [
                    inc_ref[k, c, pl.ds(base + g * SUB * words + w, SUB, stride=words), :] for g in range(groups)
                ]
                for b in range(BITS):
                    total = None
                    for g in range(groups):
                        term = jnp.where(jnp.bitwise_and(word[g], 1 << b) != 0, cost[g], 0.0)
                        total = term if total is None else total + term
                    row = (w * BITS + b) * SUB
                    if first:
                        acc[k, c, row:row + SUB, :] = total
                    else:
                        acc[k, c, row:row + SUB, :] += total

    def skim_finish(k):
        count = words * BITS
        ones = jnp.ones((SUB, LANES), jnp.float32)
        for c in range(class_local):
            rows = None
            for s in range(SUB):
                value = acc[k, c, pl.ds(s, count, stride=SUB), :]
                rows = value if rows is None else rows + value
            summed = lax.dot_general(
                ones, rows, (((1,), (1,)), ((), ())),
                precision=lax.Precision.HIGHEST, preferred_element_type=jnp.float32,
            )
            skim_out[k, c:c + 1, :] = summed[0:1, :]

    def reduce_pair(k):
        aon_own[k] = aon_own[k] + pair_buf[k]

    def aon_sum(k):
        total = aon_own[k, 0]
        for j in range(1, half):
            total = total + rs_buf[k, j]
        aon_total[k] = total

    def next_flow(k):
        step = step_ref[k]
        for c in range(class_local):
            now = flow_of(k, c)
            flows_all[k + 1, my_cls, pl.ds(c, link_rows, stride=class_local), :] = now + step * (aon_total[k, c] - now)

    def partials(k):
        cost = path = None
        for c in range(class_local):
            value = times[k, 0, 0, c]
            a, b = fold_rows(value * flow_of(k, c)), fold_rows(value * aon_total[k, c])
            cost = a if cost is None else cost + a
            path = b if path is None else path + b
        part_one[my_cls, 2 * k] = cost
        part_one[my_cls, 2 * k + 1] = path

    flows_all[0, my_cls] = flow_ref[...]
    aon_chunks(0, other, aon_pair)
    pl.semaphore_wait(barrier, n_org - 1 + n_cls - 1)
    pair0 = pair_copy(0)
    flow0 = flow_copies(0, flow_ref)
    aon_chunks(0, core, aon_own)
    pair0.wait()
    reduce_pair(0)
    rs0 = rs_copies(0)
    for made in flow0:
        made.wait()
    for c in range(class_local):
        times[0, 0, 0, c] = link_time(0, c)
    time0 = time_copies(0)
    aon_chunks(1, other, aon_pair)
    pair1 = pair_copy(1)
    aon_chunks(1, core, aon_own)
    pair1.wait()
    reduce_pair(1)
    rs1 = rs_copies(1)
    skim_chunk(0, 0, 0, True)
    for made in rs0:
        made.wait()
    aon_sum(0)
    next_flow(0)
    flow1 = flow_copies(1, flows_all.at[1, my_cls])
    time0[0].wait()
    forward0 = []
    for j in range(1, half):
        time0[j].wait()
        forward0.append(forward(0, j))
    skim_chunk(0, 0, 1, False)
    for j in range(1, half):
        skim_chunk(0, j, 0, False)
    for made in flow1:
        made.wait()
    for c in range(class_local):
        times[1, 0, 0, c] = link_time(1, c)
    time1 = time_copies(1)
    for made in rs1:
        made.wait()
    aon_sum(1)
    next_flow(1)
    flow2 = flow_copies(2, flows_all.at[2, my_cls])
    partials(0)
    partials(1)
    first_sums = [
        copy(part_one.at[my_cls], part_one.at[my_cls], one_send.at[i], one_recv.at[i], {"cls": (my_cls + i) % n_cls})
        for i in range(1, n_cls)
    ]
    flow_out[...] = flows_all[2, my_cls]
    for j in range(1, half):
        forward0[j - 1].wait()
        skim_chunk(0, j, 1, False)
    skim_finish(0)
    skim_chunk(1, 0, 0, True)
    time1[0].wait()
    forward1 = []
    for j in range(1, half):
        time1[j].wait()
        forward1.append(forward(1, j))
    for made in first_sums:
        made.wait()
    total = part_one[0]
    for i in range(1, n_cls):
        total = total + part_one[i]
    part_two[my_org] = total
    second_sums = [
        copy(part_two.at[my_org], part_two.at[my_org], two_send.at[i], two_recv.at[i], {"org": (my_org + i) % n_org})
        for i in range(1, n_org)
    ]
    skim_chunk(1, 0, 1, False)
    for j in range(1, half):
        skim_chunk(1, j, 0, False)
    for made in flow2:
        made.wait()
    for c in range(class_local):
        cost_out[pl.ds(c, link_rows, stride=class_local), :] = link_time(2, c)
    for j in range(1, half):
        forward1[j - 1].wait()
        skim_chunk(1, j, 1, False)
    skim_finish(1)
    for made in second_sums:
        made.wait()
    total = part_two[0]
    for i in range(1, n_org):
        total = total + part_two[i]
    lanes_out = lax.broadcasted_iota(jnp.int32, (1, LANES), 1)
    gaps = jnp.zeros((1, LANES), jnp.float32)
    for k in range(iters):
        cost = jnp.sum(jnp.sum(total[2 * k], axis=0, keepdims=True), axis=1, keepdims=True)
        path = jnp.sum(jnp.sum(total[2 * k + 1], axis=0, keepdims=True), axis=1, keepdims=True)
        gaps = jnp.where(lanes_out == k, (cost - path) / cost, gaps)
    gap_out[...] = gaps[:, :iters]


def shards(n_cls, n_org, flows_start, interaction, free_time, capacity, demand, incidence, step_size):
    class_local, link_shard = flows_start.shape
    class_count = interaction.shape[1]
    iters, _, anchors, words, links = incidence.shape
    assert iters == 2 and anchors == 1 and class_count == n_cls * class_local
    link_rows = link_shard // LANES
    half = n_org // 2

    def interleave(x):
        lead = x.shape[:-2]
        rows, cols = x.shape[-2:]
        x = x.reshape(lead + (rows, cols // LANES, LANES))
        return jnp.swapaxes(x, -3, -2).reshape(lead + (rows * cols // LANES, LANES))

    def restore(x):
        x = x.reshape(link_rows, class_local, LANES)
        return jnp.swapaxes(x, 0, 1).reshape(class_local, link_shard)

    inc = interleave(incidence.reshape(iters, class_local, words, links))
    vmem = pl.BlockSpec(memory_space=pltpu.VMEM)
    smem = pl.BlockSpec(memory_space=pltpu.SMEM)
    f32 = jnp.float32
    tile = (class_local, link_rows, LANES)
    dma = pltpu.SemaphoreType.DMA
    count = demand.shape[2]
    outs = pl.pallas_call(
        functools.partial(kernel, n_cls, n_org, iters, class_local, words, link_rows),
        out_shape=(
            jax.ShapeDtypeStruct((class_local * link_rows, LANES), f32),
            jax.ShapeDtypeStruct((class_local * link_rows, LANES), f32),
            jax.ShapeDtypeStruct((iters, class_local, count), f32),
            jax.ShapeDtypeStruct((1, iters), f32),
        ),
        in_specs=[vmem] * 6 + [smem],
        out_specs=(vmem,) * 4,
        scratch_shapes=[
            pltpu.VMEM((iters + 1, n_cls, class_local * link_rows, LANES), f32),
            pltpu.VMEM((iters, half) + tile, f32),
            pltpu.VMEM((iters, half) + tile, f32),
            pltpu.VMEM((iters, half) + tile, f32),
            pltpu.VMEM((iters, half) + tile, f32),
            pltpu.VMEM((iters,) + tile, f32),
            pltpu.VMEM((iters, half, 2) + tile, f32),
            pltpu.VMEM((iters, class_local, words * BITS * SUB, LANES), f32),
            pltpu.VMEM((n_cls, 2 * iters, SUB, LANES), f32),
            pltpu.VMEM((n_org, 2 * iters, SUB, LANES), f32),
            dma((iters + 1, n_cls)), dma((iters + 1, n_cls)),
            dma((iters,)), dma((iters,)),
            dma((iters, half)), dma((iters, half)),
            dma((iters, half)), dma((iters, half)),
            dma((iters, half)), dma((iters, half)),
            dma((n_cls,)), dma((n_cls,)),
            dma((n_org,)), dma((n_org,)),
        ],
        compiler_params=pltpu.CompilerParams(collective_id=0, has_side_effects=True),
    )(
        interleave(flows_start), interleave(interaction), interleave(free_time),
        capacity.reshape(link_rows, LANES), demand.reshape(class_local, count), inc, step_size,
    )
    flows, costs, skims, gaps = outs
    return restore(flows), restore(costs), skims.reshape(iters, class_local, anchors, count), gaps.reshape(iters)


def solution(mesh):
    placed = (
        P("cls", "org"),
        P("cls", None, "org"),
        P("cls", "org"),
        P("org"),
        P("cls", "org", None),
        P(None, "cls", "org", None, None),
        P(),
    )
    return jax.shard_map(
        functools.partial(shards, mesh.shape["cls"], mesh.shape["org"]),
        mesh=mesh,
        in_specs=placed,
        out_specs=(P("cls", "org"), P("cls", "org"), P(None, "cls", "org", None), P()),
        check_vma=False,
    )
```

```python
import functools

import jax
import jax.numpy as jnp
from jax import lax
from jax.experimental import pallas as pl
from jax.experimental.pallas import tpu as pltpu
from jax.sharding import PartitionSpec as P

BITS = 30
TRIP_BITS = 4
LANES = 128
SUB = 8
MESH = pl.DeviceIdType.MESH


def kernel(
    n_cls, n_org, iters, class_local, words, link_rows,
    flow_ref, inter_hbm, free_ref, cap_ref, demand_ref, inc_hbm, step_ref,
    flow_out, cost_out, skim_out, gap_out,
    inc_ref, inter_ref, flows_all, aon, aon_recv, times, acc, part_one, part_two,
    inc_sem, inter_sem, flow_send, flow_recv, pair_send, pair_recv, rs_send, rs_recv,
    time_send, time_recv, one_send, one_recv, two_send, two_recv,
):
    my_cls = lax.axis_index("cls")
    my_org = lax.axis_index("org")
    groups = link_rows // SUB
    class_count = n_cls * class_local
    levels = [1 << i for i in range(n_org.bit_length() - 1)]

    def across(mask):
        place = my_org
        for level in levels:
            if mask & level:
                place = place + level * (1 - 2 * ((my_org // level) % 2))
        return place

    loads = [pltpu.make_async_copy(inc_hbm.at[k], inc_ref.at[k], inc_sem.at[k]) for k in range(iters)]
    inter_load = pltpu.make_async_copy(inter_hbm, inter_ref, inter_sem)
    loads[0].start()
    loads[1].start()
    inter_load.start()

    barrier = pltpu.get_barrier_semaphore()
    for i in range(1, n_org):
        pl.semaphore_signal(barrier, inc=1, device_id={"org": (my_org + i) % n_org}, device_id_type=MESH)
    for i in range(1, n_cls):
        pl.semaphore_signal(barrier, inc=1, device_id={"cls": (my_cls + i) % n_cls}, device_id_type=MESH)

    demand = demand_ref[...]
    lane = lax.broadcasted_iota(jnp.int32, demand.shape, 1)
    spot = lane % BITS
    low_half = BITS // 2
    masks = {}
    for bit in range(TRIP_BITS):
        chosen = jnp.bitwise_and(jnp.right_shift(demand, bit), 1)
        for w in range(words):
            inside = lane // BITS == w
            low = jnp.where(inside & (spot < low_half), jnp.left_shift(chosen, spot % low_half), 0)
            high = jnp.where(inside & (spot >= low_half), jnp.left_shift(chosen, spot % low_half), 0)
            low_sum = jnp.sum(low.astype(jnp.float32), axis=1, keepdims=True).astype(jnp.int32)
            high_sum = jnp.sum(high.astype(jnp.float32), axis=1, keepdims=True).astype(jnp.int32)
            both = low_sum + jnp.left_shift(high_sum, low_half)
            for c in range(class_local):
                masks[bit, w, c] = jnp.broadcast_to(both[c:c + 1, :], (SUB, LANES))

    def aon_chunks(k, parity):
        core = my_org % 2
        place = core + parity * (1 - 2 * core)

        def one(h, carry):
            upper = 0
            for level in levels[1:]:
                mine = (my_org // level) % 2
                wanted = (h // (level // 2)) % 2
                upper = upper + level * ((mine + wanted) % 2)
            base = (upper + place) * (link_rows * words)
            for c in range(class_local):
                for g in range(groups):
                    word = [
                        inc_ref[k, c, pl.ds(base + g * SUB * words + w, SUB, stride=words), :]
                        for w in range(words)
                    ]
                    total = None
                    for bit in range(TRIP_BITS):
                        count = None
                        for w in range(words):
                            ones = lax.population_count(jnp.bitwise_and(word[w], masks[bit, w, c]))
                            count = ones if count is None else count + ones
                        count = jnp.left_shift(count, bit)
                        total = count if total is None else total + count
                    aon[k, parity, h, c, g * SUB:(g + 1) * SUB, :] = total.astype(jnp.float32)
            return carry

        lax.fori_loop(0, n_org // 2, one, 0)

    def copy(src, dst, send, recv, device):
        made = pltpu.make_async_remote_copy(
            src_ref=src, dst_ref=dst, send_sem=send, recv_sem=recv, device_id=device, device_id_type=MESH
        )
        made.start()
        return made

    def pair_copy(k):
        return copy(aon.at[k, 1], aon_recv.at[k, 1], pair_send.at[k], pair_recv.at[k], {"org": across(1)})

    def load_send(k, r):
        level = r & -r
        return copy(aon.at[k, 0, r // 2], aon_recv.at[k, 0, r // 2], rs_send.at[k, r], rs_recv.at[k, r],
                    {"org": across(level)})

    def load_join(k, r):
        held = r - (r & -r)
        aon[k, 0, held // 2] += aon_recv[k, 0, r // 2]

    def time_sends(k, m):
        sent = {}
        low = (m & -m) if m else n_org
        for level in reversed(levels):
            if level < low:
                to = m + level
                sent[to] = copy(times.at[k, m], times.at[k, to], time_send.at[k, to], time_recv.at[k, to],
                                {"org": across(level)})
        return sent

    def flow_copies(k, src):
        return [
            copy(src, flows_all.at[k, my_cls], flow_send.at[k, i], flow_recv.at[k, i], {"cls": (my_cls + i) % n_cls})
            for i in range(1, n_cls)
        ]

    def flow_of(k, c):
        return flows_all[k, my_cls, pl.ds(c, link_rows, stride=class_local), :]

    def link_time(k, c):
        load = None
        for e in range(class_count):
            weight = inter_ref[c, pl.ds(e, link_rows, stride=class_count), :]
            flow = flows_all[k, e // class_local, pl.ds(e % class_local, link_rows, stride=class_local), :]
            term = weight * flow
            load = term if load is None else load + term
        ratio = load / cap_ref[...]
        square = ratio * ratio
        return free_ref[pl.ds(c, link_rows, stride=class_local), :] * (1.0 + 0.15 * square * square)

    def fold_rows(value):
        return jnp.sum(value.reshape(groups, SUB, LANES), axis=0)

    def skim_chunk(k, m):
        first = m == 0
        base = across(m) * (link_rows * words)
        for c in range(class_local):
            cost = [times[k, m, c, g * SUB:(g + 1) * SUB, :] for g in range(groups)]
            for w in range(words):
                word = [
                    inc_ref[k, c, pl.ds(base + g * SUB * words + w, SUB, stride=words), :] for g in range(groups)
                ]
                for b in range(BITS):
                    total = None
                    for g in range(groups):
                        term = jnp.where(jnp.bitwise_and(word[g], 1 << b) != 0, cost[g], 0.0)
                        total = term if total is None else total + term
                    row = (w * BITS + b) * SUB
                    if first:
                        acc[k, c, row:row + SUB, :] = total
                    else:
                        acc[k, c, row:row + SUB, :] += total

    def skim_finish(k):
        count = words * BITS
        ones = jnp.ones((SUB, LANES), jnp.float32)
        for c in range(class_local):
            rows = None
            for s in range(SUB):
                value = acc[k, c, pl.ds(s, count, stride=SUB), :]
                rows = value if rows is None else rows + value
            summed = lax.dot_general(
                ones, rows, (((1,), (1,)), ((), ())),
                precision=lax.Precision.HIGHEST, preferred_element_type=jnp.float32,
            )
            skim_out[k, c:c + 1, :] = summed[0:1, :]

    def next_flow(k):
        step = step_ref[k]
        for c in range(class_local):
            now = flow_of(k, c)
            flows_all[k + 1, my_cls, pl.ds(c, link_rows, stride=class_local), :] = now + step * (aon[k, 0, 0, c] - now)

    def partials(k):
        cost = path = None
        for c in range(class_local):
            value = times[k, 0, c]
            a, b = fold_rows(value * flow_of(k, c)), fold_rows(value * aon[k, 0, 0, c])
            cost = a if cost is None else cost + a
            path = b if path is None else path + b
        part_one[my_cls, 2 * k] = cost
        part_one[my_cls, 2 * k + 1] = path

    def halve_first(k):
        aon[k, 0] = aon[k, 0] + aon_recv[k, 1]
        return {r: load_send(k, r) for r in reversed(range(2, n_org, 2)) if r & -r == 2}

    def halve_next(k, sent, level):
        for r in sorted(sent, reverse=True):
            held = r - (r & -r)
            if r & -r == level // 2 and held:
                sent[r].wait()
                load_join(k, r)
                if held & -held == level:
                    sent[held] = load_send(k, held)

    def halve_last(k, sent):
        for level in levels[1:]:
            sent[level].wait()
            load_join(k, level)

    def costs_ready(k):
        for c in range(class_local):
            times[k, 0, c] = link_time(k, c)
        return time_sends(k, 0)

    def wait_all(group):
        for made in group:
            made.wait()

    order = sorted(range(1, n_org), key=lambda m: (m % 2, bin(m).count("1"), m))
    even = [m for m in order if m % 2 == 0]
    odd = [m for m in order if m % 2 == 1]

    loads[0].wait()
    aon_chunks(0, 1)
    pl.semaphore_wait(barrier, n_org - 1 + n_cls - 1)
    pair0 = pair_copy(0)
    flow0 = flow_copies(0, flow_ref)
    flows_all[0, my_cls] = flow_ref[...]
    aon_chunks(0, 0)
    pair0.wait()
    sums0 = halve_first(0)
    loads[1].wait()
    aon_chunks(1, 1)
    pair1 = pair_copy(1)
    aon_chunks(1, 0)
    for level in levels[2:]:
        halve_next(0, sums0, level)
    pair1.wait()
    sums1 = halve_first(1)
    inter_load.wait()
    wait_all(flow0)
    sent0 = costs_ready(0)
    halve_last(0, sums0)
    next_flow(0)
    flow1 = flow_copies(1, flows_all.at[1, my_cls])
    for level in levels[2:]:
        halve_next(1, sums1, level)
    for m in even:
        sent0[m].wait()
        sent0.update(time_sends(0, m))
    skim_chunk(0, 0)
    wait_all(flow1)
    sent1 = costs_ready(1)
    halve_last(1, sums1)
    next_flow(1)
    flow2 = flow_copies(2, flows_all.at[2, my_cls])
    partials(0)
    partials(1)
    first_sums = [
        copy(part_one.at[my_cls], part_one.at[my_cls], one_send.at[i], one_recv.at[i], {"cls": (my_cls + i) % n_cls})
        for i in range(1, n_cls)
    ]
    flow_out[...] = flows_all[2, my_cls]
    middle = even[len(even) // 2:]
    for m in even[:len(even) // 2]:
        skim_chunk(0, m)
    for m in even:
        sent1[m].wait()
        sent1.update(time_sends(1, m))
        if m in middle:
            skim_chunk(0, m)
    wait_all(first_sums)
    total = part_one[0]
    for i in range(1, n_cls):
        total = total + part_one[i]
    part_two[my_org] = total
    second_sums = [
        copy(part_two.at[my_org], part_two.at[my_org], two_send.at[i], two_recv.at[i], {"org": (my_org + i) % n_org})
        for i in range(1, n_org)
    ]
    for m in odd:
        sent0[m].wait()
        skim_chunk(0, m)
    skim_finish(0)
    for m in [0] + even:
        skim_chunk(1, m)
    wait_all(flow2)
    for c in range(class_local):
        cost_out[pl.ds(c, link_rows, stride=class_local), :] = link_time(2, c)
    for m in odd:
        sent1[m].wait()
        skim_chunk(1, m)
    skim_finish(1)
    wait_all(second_sums)
    total = part_two[0]
    for i in range(1, n_org):
        total = total + part_two[i]
    lanes_out = lax.broadcasted_iota(jnp.int32, (1, LANES), 1)
    gaps = jnp.zeros((1, LANES), jnp.float32)
    for k in range(iters):
        cost = jnp.sum(jnp.sum(total[2 * k], axis=0, keepdims=True), axis=1, keepdims=True)
        path = jnp.sum(jnp.sum(total[2 * k + 1], axis=0, keepdims=True), axis=1, keepdims=True)
        gaps = jnp.where(lanes_out == k, (cost - path) / cost, gaps)
    gap_out[...] = gaps[:, :iters]


def hand_over(*refs):
    count = len(refs) // 2
    for source, target in zip(refs[:count], refs[count:]):
        target[...] = source[...]


def shards(n_cls, n_org, flows_start, interaction, free_time, capacity, demand, incidence, step_size):
    class_local, link_shard = flows_start.shape
    class_count = interaction.shape[1]
    iters, _, anchors, words, links = incidence.shape
    assert iters == 2 and anchors == 1 and class_count == n_cls * class_local
    link_rows = link_shard // LANES

    def interleave(x):
        lead = x.shape[:-2]
        rows, cols = x.shape[-2:]
        x = x.reshape(lead + (rows, cols // LANES, LANES))
        return jnp.swapaxes(x, -3, -2).reshape(lead + (rows * cols // LANES, LANES))

    def restore(x):
        x = x.reshape(link_rows, class_local, LANES)
        return jnp.swapaxes(x, 0, 1).reshape(class_local, link_shard)

    inc = interleave(incidence.reshape(iters, class_local, words, links))
    vmem = pl.BlockSpec(memory_space=pltpu.VMEM)
    hbm = pl.BlockSpec(memory_space=pl.ANY)
    smem = pl.BlockSpec(memory_space=pltpu.SMEM)
    f32 = jnp.float32
    tile = (class_local, link_rows, LANES)
    dma = pltpu.SemaphoreType.DMA
    count = demand.shape[2]
    outs = pl.pallas_call(
        functools.partial(kernel, n_cls, n_org, iters, class_local, words, link_rows),
        out_shape=(
            jax.ShapeDtypeStruct((class_local * link_rows, LANES), f32),
            jax.ShapeDtypeStruct((class_local * link_rows, LANES), f32),
            jax.ShapeDtypeStruct((iters, class_local, count), f32),
            jax.ShapeDtypeStruct((1, iters), f32),
        ),
        in_specs=[vmem, hbm, vmem, vmem, vmem, hbm, smem],
        out_specs=(vmem,) * 4,
        scratch_shapes=[
            pltpu.VMEM((iters, class_local, words * links // LANES, LANES), jnp.int32),
            pltpu.VMEM((class_local, class_count * link_rows, LANES), f32),
            pltpu.VMEM((iters + 1, n_cls, class_local * link_rows, LANES), f32),
            pltpu.VMEM((iters, 2, n_org // 2) + tile, f32),
            pltpu.VMEM((iters, 2, n_org // 2) + tile, f32),
            pltpu.VMEM((iters, n_org) + tile, f32),
            pltpu.VMEM((iters, class_local, words * BITS * SUB, LANES), f32),
            pltpu.VMEM((n_cls, 2 * iters, SUB, LANES), f32),
            pltpu.VMEM((n_org, 2 * iters, SUB, LANES), f32),
            dma((iters,)), dma,
            dma((iters + 1, n_cls)), dma((iters + 1, n_cls)),
            dma((iters,)), dma((iters,)),
            dma((iters, n_org)), dma((iters, n_org)),
            dma((iters, n_org)), dma((iters, n_org)),
            dma((n_cls,)), dma((n_cls,)),
            dma((n_org,)), dma((n_org,)),
        ],
        compiler_params=pltpu.CompilerParams(collective_id=0, has_side_effects=True),
    )(
        interleave(flows_start), interleave(interaction), interleave(free_time),
        capacity.reshape(link_rows, LANES), demand.reshape(class_local, count), inc, step_size,
    )
    flows, costs, skims, gaps = pl.pallas_call(
        hand_over,
        out_shape=tuple(jax.ShapeDtypeStruct(x.shape, x.dtype) for x in outs),
        in_specs=[vmem] * len(outs),
        out_specs=(vmem,) * len(outs),
    )(*outs)
    return restore(flows), restore(costs), skims.reshape(iters, class_local, anchors, count), gaps.reshape(iters)


def solution(mesh):
    placed = (
        P("cls", "org"),
        P("cls", None, "org"),
        P("cls", "org"),
        P("org"),
        P("cls", "org", None),
        P(None, "cls", "org", None, None),
        P(),
    )
    return jax.shard_map(
        functools.partial(shards, mesh.shape["cls"], mesh.shape["org"]),
        mesh=mesh,
        in_specs=placed,
        out_specs=(P("cls", "org"), P("cls", "org"), P(None, "cls", "org", None), P()),
        check_vma=False,
    )
```
